256 devices in a mesh: chip: 8 (over y, core), board: 8 (over z), cuts: 4 (over x).
Axes of the slice: x: 4, y: 4, z: 8, core: 2. Of those that a mesh axis runs over, the one named last changes fastest.
Arguments:
- features: bfloat16 [256, 2048, 1024], P(('chip', 'board', 'cuts')), may hold values from -6 to 6
- targets: bfloat16 [256, 2048, 256], P(('chip', 'board', 'cuts')), may hold values from -24 to 24
- lower_weight: bfloat16 [256, 1024, 512], P(('chip', 'board', 'cuts')), may hold values from -0.1875 to 0.1875
- head_weight: float32 [256, 512, 256], P(('chip', 'board', 'cuts')), may hold values from -0.25 to 0.25
- batch_rows: int32 [256, 2, 1024], P(('chip', 'board', 'cuts')), may hold values from 0 to 2047
- sample_counts: int32 [256], P(('chip', 'board', 'cuts')), may hold values from 1 to 1000
- cluster_ids: int32 [256], P(('chip', 'board', 'cuts')), may hold values from 0 to 7, as said below
Outputs:
- cluster_step: float32 [256, 512, 256], P(('chip', 'board', 'cuts'))
The draws below stay inside these ranges and needn't reach their ends.
Inputs may be any that keep to these rules, and one draw needn't show every extreme that they name: `cluster_ids`: every one of the 8 clusters has at least one client.
All inputs are finite; a program needn't handle non-finite values.
Results may differ from the reference program's by a relative error of at most 0.0003.
Values sent between devices are 32-bit elements; how exact they have to be, the bound alone decides.
A program may use at most 64 MiB of HBM per device.

```python
import jax
import jax.numpy as jnp
from jax import lax

IN = 1024
HID = 512
OUT = 256
CLUSTERS = 8
STEPS = 2
POOL = 2048
ROWS = 1024
CLIENTS = 256


def draw_cluster_ids(key, part):
    first = jax.random.fold_in(key, 11)
    second = jax.random.fold_in(key, 23)
    drawn = jax.random.randint(first, (CLIENTS,), 0, CLUSTERS, dtype=jnp.int32)
    order = jax.random.permutation(second, CLIENTS)
    return drawn.at[order[:CLUSTERS]].set(jnp.arange(CLUSTERS, dtype=jnp.int32))


def with_ends(values, rng, smallest, largest):
    index_at = [jax.random.randint(jax.random.fold_in(rng, axis), (), 0, length) for axis, length in enumerate(values.shape)]
    widest = values.shape.index(max(values.shape))
    neighbour = index_at[:widest] + [(index_at[widest] + 1) % values.shape[widest]] + index_at[widest + 1:]
    return values.at[tuple(index_at)].set(smallest).at[tuple(neighbour)].set(largest)


def level_of(key, shape, cuts, low, largest):
    def one(dim, parts):
        draws = jax.random.uniform(jax.random.fold_in(jax.random.fold_in(key, 6), dim), (parts,), jnp.float32, low / len(cuts), largest / len(cuts))
        return jnp.repeat(jnp.exp(draws), shape[dim] // parts).reshape((-1,) + (1,) * (len(shape) - dim - 1))

    gain = one(*cuts[0])
    for cut in cuts[1:]:
        gain = gain * one(*cut)
    return gain


def centred(key, shape, width, limit, cuts=(), kind=jnp.bfloat16):
    result = jax.random.normal(key, shape, jnp.float32) * width
    if len(cuts) > 0:
        result = level_of(key, shape, cuts, -0.22, 0.18) * result
    return jnp.clip(result, min=-limit, max=limit).astype(kind)


def setup_inputs(seed: int = 0) -> dict:
    arg_keys = jax.random.split(jax.random.key(seed), 8)
    return {
        "features": centred(arg_keys[0], (CLIENTS, POOL, IN), 1.0, 6.0, ((0, 256),)),
        "targets": centred(arg_keys[1], (CLIENTS, POOL, OUT), 4.0, 24.0, ((0, 256),)),
        "lower_weight": centred(arg_keys[2], (CLIENTS, IN, HID), IN ** -0.5, 0.1875, ((0, 256),)),
        "head_weight": centred(arg_keys[3], (CLIENTS, HID, OUT), HID ** -0.5, 0.25, ((0, 256),), jnp.float32),
        "batch_rows": with_ends(jax.random.randint(arg_keys[4], (CLIENTS, STEPS, ROWS), 0, POOL), jax.random.fold_in(arg_keys[4], 1), 0, POOL - 1).astype(jnp.int32),
        "sample_counts": with_ends(jax.random.randint(arg_keys[5], (CLIENTS,), 1, 1001), jax.random.fold_in(arg_keys[5], 1), 1, 1000).astype(jnp.int32),
        "cluster_ids": draw_cluster_ids(jax.random.fold_in(arg_keys[7], 71), 0),
    }


LR = 0.5


def one_client(args):
    feats, targs, lower, head, rows = args
    hidden = jnp.tanh(jnp.dot(feats, lower, preferred_element_type=jnp.float32))
    weight = head
    for step in range(STEPS):
        picked = jnp.take(hidden, rows[step], axis=0)
        wanted = jnp.take(targs, rows[step], axis=0).astype(jnp.float32)
        err = jnp.dot(picked, weight, precision=lax.Precision.HIGHEST) - wanted
        grad = jnp.dot(picked.T, err, precision=lax.Precision.HIGHEST) / ROWS
        weight = weight - LR * grad
    return weight - head


def reference(features, targets, lower_weight, head_weight, batch_rows, sample_counts, cluster_ids):
    deltas = lax.map(one_client, (features, targets, lower_weight, head_weight, batch_rows))
    onehot = (cluster_ids[:, None] == jnp.arange(CLUSTERS, dtype=jnp.int32)[None, :]).astype(jnp.float32)
    weighted = onehot * sample_counts.astype(jnp.float32)[:, None]
    flat = deltas.reshape(CLIENTS, HID * OUT)
    sums = jnp.dot(weighted.T, flat, precision=lax.Precision.HIGHEST)
    counts = jnp.sum(weighted, axis=0)
    mine = jnp.take(sums, cluster_ids, axis=0).reshape(CLIENTS, HID, OUT)
    denom = jnp.take(counts, cluster_ids, axis=0)
    return mine / (LR * denom)[:, None, None]
```

```python
import functools
import jax
import jax.numpy as jnp
from jax import lax
from jax.experimental import pallas as pl
from jax.experimental.pallas import tpu as pltpu
from jax.sharding import Mesh
from jax.sharding import PartitionSpec as P

CHIP = ("chip_0", "chip_1")
CHIP_BOARD_CUTS = ("chip_0", "chip_1", "board", "cuts")


LR = 0.5


def laid_out(blocks, dim):
    blocks = jnp.moveaxis(blocks, 0, dim)
    dims = blocks.shape
    return blocks.reshape(*dims[:dim], dims[dim] * dims[dim + 1], *dims[dim + 2 :])


def gather_in_order(value, axes, order):
    blocks = value[None]
    for k in order:
        blocks = lax.all_gather(blocks, axes[k], axis=0, tiled=True)
    block = [lax.axis_size(axes[k]) for k in reversed(order)]
    blocks = blocks.reshape(*block, *value.shape)
    turned = sorted(range(len(order)), key=lambda place: order[len(order) - 1 - place])
    return blocks.transpose(*turned, *range(len(order), blocks.ndim)).reshape(-1, *value.shape)


def gathered_by_axis(value, axes, order, dim):
    return laid_out(gather_in_order(value, axes, order), dim)


def cut_along(value, dim, peers):
    dims = value.shape
    blocks = value.reshape(*dims[:dim], peers, dims[dim] // peers, *dims[dim + 1 :])
    return jnp.moveaxis(blocks, dim, 0)


def exchange_both(value, axis, axes, splits, concats):
    sizes = [lax.axis_size(a) for a in axes]
    blocks = cut_along(value, splits[0], sizes[0])
    blocks = jnp.moveaxis(cut_along(blocks, splits[1] + 1, sizes[1]), 0, 1)
    inside = blocks.shape[2:]
    blocks = blocks.reshape(-1, *inside)
    blocks = lax.all_to_all(blocks, axis, split_axis=0, concat_axis=0, tiled=True)
    blocks = laid_out(blocks.reshape(*sizes, *inside), concats[0] + 1)
    return laid_out(blocks, concats[1])


NB=4

def split(v):
    hi = v.astype(jnp.bfloat16)
    lo = (v - hi.astype(jnp.float32)).astype(jnp.bfloat16)
    return hi, lo

NT=(((1,),(1,)),((),()))
TN=(((0,),(0,)),((),()))
def dg(a,b,d): return lax.dot_general(a,b,d,preferred_element_type=jnp.float32)

def compute(feat, targ, low, head, rows, fv, tv, lv, hv, hh, hl, cm, sems, nb=NB):
    pool = fv.shape[0]; blk = pool//nb
    cps=[pltpu.make_async_copy(low.at[0], lv, sems.at[0])]
    for b in range(nb):
        cps.append(pltpu.make_async_copy(feat.at[0,pl.ds(b*blk,blk)], fv.at[pl.ds(b*blk,blk)], sems.at[1+b]))
    ch=pltpu.make_async_copy(head.at[0], hv, sems.at[1+nb])
    ct=pltpu.make_async_copy(targ.at[0], tv, sems.at[2+nb])
    cps[0].start(); cps[1].start(); ch.start(); ct.start()
    for c in cps[2:]: c.start()
    count_rows = rows.shape[2]
    for s in range(2):
        idx = rows[0, pl.ds(s,1), :]
        lowi = idx % 128
        higi = idx // 128
        bt = (lax.broadcasted_iota(jnp.int32,(128,count_rows),0)==lowi).astype(jnp.float32).astype(jnp.bfloat16)
        at = (lax.broadcasted_iota(jnp.int32,(16,count_rows),0)==higi).astype(jnp.float32).astype(jnp.bfloat16)
        cm[s] = dg(bt, at, NT)
    cps[0].wait()
    ch.wait(); ct.wait()
    def err_scaled(s, b, hhb, hlb, wh, wl):
        e = dg(hhb,wh,NT)+dg(hlb,wh,NT)+dg(hhb,wl,NT) - tv[pl.ds(b*blk,blk)].astype(jnp.float32)
        per = blk//128
        parts=[]
        for q in range(per):
            col = cm[s,:,pl.ds(b*per+q,1)]
            parts.append(e[q*128:(q+1)*128]*col)
        e = jnp.concatenate(parts,0) if per>1 else parts[0]
        return split(e)
    def grad_t(eh, el, hhb, hlb):
        return dg(eh,hhb,TN)+dg(eh,hlb,TN)+dg(el,hhb,TN)
    w0t = hv[...].T
    wh,wl = split(w0t)
    g = None
    for b in range(nb):
        cps[1+b].wait()
        sl=pl.ds(b*blk,blk)
        h = jnp.tanh(jnp.dot(fv[sl], lv[...], preferred_element_type=jnp.float32))
        hhb,hlb = split(h)
        hh[sl]=hhb; hl[sl]=hlb
        eh,el = err_scaled(0,b,hhb,hlb,wh,wl)
        t = grad_t(eh,el,hhb,hlb)
        g = t if g is None else g+t
    k = LR/count_rows
    d1 = g*(-k)
    wh,wl = split(w0t+d1)
    g=None
    for b in range(nb):
        sl=pl.ds(b*blk,blk)
        eh,el = err_scaled(1,b,hh[sl],hl[sl],wh,wl)
        t = grad_t(eh,el,hh[sl],hl[sl])
        g = t if g is None else g+t
    return (d1 + g*(-k)).T

def scratch(nb=NB):
    return [pltpu.VMEM((2048,1024),jnp.bfloat16), pltpu.VMEM((2048,256),jnp.bfloat16), pltpu.VMEM((1024,512),jnp.bfloat16),
            pltpu.VMEM((512,256),jnp.float32), pltpu.VMEM((2048,512),jnp.bfloat16), pltpu.VMEM((2048,512),jnp.bfloat16),
            pltpu.VMEM((2,128,16),jnp.float32), pltpu.SemaphoreType.DMA((3+nb,))]

def kern(feat,targ,low,head,rows,out,*scr, nb=NB):
    out[...] = compute(feat,targ,low,head,rows,*scr,nb=nb)

def local(feat,targ,low,head,rows,nb=NB):
    A=pl.BlockSpec(memory_space=pl.ANY); V=pl.BlockSpec(memory_space=pltpu.VMEM)
    return pl.pallas_call(functools.partial(kern,nb=nb), out_shape=jax.ShapeDtypeStruct((512,256),jnp.float32),
        in_specs=[A,A,A,A,V], out_specs=V, scratch_shapes=scratch(nb),
        compiler_params=pltpu.CompilerParams(vmem_limit_bytes=48*2**20))(feat,targ,low,head,rows)


def on_device(features, targets, lower_weight, head_weight, batch_rows, sample_counts, cluster_ids):
    delta = local(features, targets, lower_weight, head_weight, batch_rows)
    cluster = cluster_ids[0]
    number = 8
    chip_count = lax.axis_size(CHIP)
    rest_count = lax.axis_size(("board", "cuts"))
    every_id, every_count = (
        gathered_by_axis(cluster_ids, CHIP_BOARD_CUTS, (0, 2, 3, 1), 0),
        gathered_by_axis(sample_counts, CHIP_BOARD_CUTS, (0, 2, 3, 1), 0),
    )
    table = (every_id[:, None] == jnp.arange(number, dtype=jnp.int32)[None, :]).astype(jnp.float32)
    weighted = table * every_count.astype(jnp.float32)[:, None]
    counts = jnp.sum(weighted, axis=0)
    scaled = (sample_counts[0].astype(jnp.float32) * delta).reshape(chip_count, rest_count, -1)
    columns = exchange_both(scaled, CHIP_BOARD_CUTS, (CHIP, ("board", "cuts")), (0, 1), (0, 1))
    columns = columns.reshape(chip_count * rest_count, -1)
    share = jnp.dot(table.T, columns, precision=lax.Precision.HIGHEST)
    outgoing = jnp.dot(table, share, precision=lax.Precision.HIGHEST)
    outgoing = outgoing.reshape(chip_count, rest_count, -1)
    arrived = exchange_both(outgoing, CHIP_BOARD_CUTS, (CHIP, ("board", "cuts")), (0, 1), (0, 1))
    mine = arrived.reshape(delta.shape)
    denom = lax.dynamic_index_in_dim(counts, cluster, 0, keepdims=False)
    return (mine / (LR * denom))[None]


def solution(mesh):
    finer = Mesh(
        mesh.devices.reshape(4, 2, mesh.shape["board"], mesh.shape["cuts"]),
        ("chip_0", "chip_1", "board", "cuts"),
    )
    return jax.shard_map(
        on_device,
        mesh=finer,
        in_specs=(
            P(CHIP_BOARD_CUTS, None, None),
            P(CHIP_BOARD_CUTS, None, None),
            P(CHIP_BOARD_CUTS, None, None),
            P(CHIP_BOARD_CUTS, None, None),
            P(CHIP_BOARD_CUTS, None, None),
            P(CHIP_BOARD_CUTS),
            P(CHIP_BOARD_CUTS),
        ),
        out_specs=P(CHIP_BOARD_CUTS, None, None),
        check_vma=False,
    )
```

```python
import functools
import math

import jax
import jax.numpy as jnp
from jax import lax
from jax.experimental import pallas as pl
from jax.experimental.pallas import tpu as pltpu
from jax.sharding import PartitionSpec as P

AXES = ("chip", "board", "cuts")
LR = 0.5
CLUSTERS = 8
LANES = 128
BLOCK = 512
PIECE = 256
MESH = pl.DeviceIdType.MESH
NN = (((1,), (0,)), ((), ()))
NT = (((1,), (1,)), ((), ()))
TN = (((0,), (0,)), ((), ()))


def product(a, b, dims):
    return lax.dot_general(a, b, dims, preferred_element_type=jnp.float32)


def split(value):
    high = value.astype(jnp.bfloat16)
    return high, (value - high.astype(jnp.float32)).astype(jnp.bfloat16)


def load_all(features, targets, lower, head, x_ref, t_ref, v_ref, w_ref, sems):
    block = min(BLOCK, x_ref.shape[0])
    blocks = x_ref.shape[0] // block
    pairs = [(lower.at[0], v_ref)]
    for k in range(blocks):
        rows = pl.ds(k * block, block)
        pairs.append((features.at[0, rows], x_ref.at[rows]))
    pairs += [(head.at[0], w_ref), (targets.at[0], t_ref)]
    copies = [pltpu.make_async_copy(src, dst, sems.at[k]) for k, (src, dst) in enumerate(pairs)]
    for copy in copies:
        copy.start()
    return copies


def count_draws(rows, m_ref):
    drawn = rows.shape[2]
    for step in range(rows.shape[1]):
        index = rows[0, pl.ds(step, 1), :]
        inner = lax.broadcasted_iota(jnp.int32, (LANES, drawn), 0) == index % LANES
        outer = lax.broadcasted_iota(jnp.int32, (m_ref.shape[2], drawn), 0) == index // LANES
        m_ref[step] = product(
            inner.astype(jnp.float32).astype(jnp.bfloat16),
            outer.astype(jnp.float32).astype(jnp.bfloat16),
            NT,
        )


def hidden_rows(copies, x_ref, v_ref, hh_ref, hl_ref):
    copies[0].wait()
    blocks = len(copies) - 3
    block = x_ref.shape[0] // blocks
    for k in range(blocks):
        copies[1 + k].wait()
        rows = pl.ds(k * block, block)
        hh_ref[rows], hl_ref[rows] = split(jnp.tanh(product(x_ref[rows], v_ref[...], NN)))


def local_step(step, weight, m_ref, t_ref, hh_ref, hl_ref, eh_ref, el_ref, drawn):
    wh, wl = split(weight)
    pool = hh_ref.shape[0]
    piece = min(PIECE, pool)
    per = piece // LANES
    for k in range(pool // piece):
        rows = pl.ds(k * piece, piece)
        high, low = hh_ref[rows], hl_ref[rows]
        err = product(high, wh, NN) + product(low, wh, NN) + product(high, wl, NN)
        err = err - t_ref[rows].astype(jnp.float32)
        err = jnp.concatenate(
            [
                err[q * LANES : (q + 1) * LANES] * m_ref[step, :, pl.ds(k * per + q, 1)]
                for q in range(per)
            ],
            0,
        )
        eh_ref[rows], el_ref[rows] = split(err)
    high, low = eh_ref[...], el_ref[...]
    grad = product(high, hh_ref[...], TN) + product(high, hl_ref[...], TN)
    grad = grad + product(low, hh_ref[...], TN)
    return grad.T * (-LR / drawn)


def kernel(
    sizes,
    features, targets, lower, head, rows, count, cluster,
    out,
    x_ref, t_ref, v_ref, w_ref, hh_ref, hl_ref, eh_ref, el_ref, m_ref,
    delta, mine, meta, part, parts, got1, sums, got2, totals, picked,
    load_sems, meta_send, meta_recv, part_send, part_recv,
    send1, recv1, send2, recv2, send3, recv3, send4, recv4,
):
    nc, nb, nx = sizes
    plane = nc * nx
    chunks = delta.shape[0]
    share = delta.shape[1] // plane
    c, b, x = (lax.axis_index(a) for a in AXES)
    me = c * nx + x

    def ahead(d):
        return (lax.rem(c + d // nx, nc), b, lax.rem(x + lax.rem(d, nx), nx))

    def behind(d):
        return (lax.rem(c + nc - d // nx, nc), b, lax.rem(x + nx - lax.rem(d, nx), nx))

    def along(e):
        return (c, lax.rem(b + e, nb), x)

    def remote(src, dst, send, recv, device):
        return pltpu.make_async_remote_copy(
            src_ref=src, dst_ref=dst, send_sem=send, recv_sem=recv, device_id=device, device_id_type=MESH
        )

    def loop(lo, hi, body):
        def run(k, carry):
            body(k)
            return carry

        lax.fori_loop(lo, hi, run, 0)

    copies = load_all(features, targets, lower, head, x_ref, t_ref, v_ref, w_ref, load_sems)
    barrier = pltpu.get_barrier_semaphore()
    loop(1, plane, lambda d: pl.semaphore_signal(barrier, inc=1, device_id=ahead(d), device_id_type=MESH))
    loop(1, nb, lambda e: pl.semaphore_signal(barrier, inc=1, device_id=along(e), device_id_type=MESH))
    count_draws(rows, m_ref)
    hidden_rows(copies, x_ref, v_ref, hh_ref, hl_ref)
    copies[-2].wait()
    copies[-1].wait()
    drawn = rows.shape[2]
    start = w_ref[...]
    first = local_step(0, start, m_ref, t_ref, hh_ref, hl_ref, eh_ref, el_ref, drawn)

    place = lax.broadcasted_iota(jnp.int32, mine.shape, 0) == cluster[0]
    mine[...] = jnp.where(place, count[0].astype(jnp.float32), 0.0)
    pl.semaphore_wait(barrier, plane - 1 + nb - 1)
    def meta_copy(d, device):
        return remote(mine, meta.at[d - 1], meta_send, meta_recv.at[d - 1], device)

    loop(1, plane, lambda d: meta_copy(d, ahead(d)).start())

    change = first + local_step(1, start + first, m_ref, t_ref, hh_ref, hl_ref, eh_ref, el_ref, drawn)
    for h in range(chunks):
        delta[h] = change[:, h * LANES : (h + 1) * LANES]

    def copy1(h, d):
        peer = ahead(d)
        at = pl.multiple_of((peer[0] * nx + peer[2]) * share, share)
        return remote(delta.at[h, pl.ds(at, share)], got1.at[h, d - 1], send1.at[h], recv1.at[h, d - 1], peer)

    for h in range(chunks):
        loop(1, plane, lambda d: copy1(h, d).start())

    def add_meta(d, total):
        meta_copy(d, ahead(d)).wait_recv()
        return total + meta[d - 1]

    part[...] = lax.fori_loop(1, plane, add_meta, mine[...])

    def part_copy(e):
        return remote(part, parts.at[e - 1], part_send, part_recv.at[e - 1], along(e))

    loop(1, nb, lambda e: part_copy(e).start())

    own = pl.multiple_of(me * share, share)

    def copy2(h, e):
        peer = along(e)
        return remote(sums.at[h, peer[1]], got2.at[h, e - 1], send2.at[h], recv2.at[h, e - 1], peer)

    for h in range(chunks):
        def add_share(d, acc):
            copy1(h, d).wait_recv()
            value = got1[h, d - 1]
            return tuple(a + value * meta[d - 1, pl.ds(k, 1), :] for k, a in enumerate(acc))

        value = delta[h, pl.ds(own, share)]
        acc = tuple(value * mine[pl.ds(k, 1), :] for k in range(CLUSTERS))
        acc = lax.fori_loop(1, plane, add_share, acc)
        for k in range(CLUSTERS):
            sums[h, k] = acc[k]
        loop(1, nb, lambda e: copy2(h, e).start())

    def copy3(h, e):
        return remote(totals.at[h, b], totals.at[h, b], send3.at[h], recv3.at[h, e - 1], along(e))

    for h in range(chunks):
        def add_sum(e, acc):
            copy2(h, e).wait_recv()
            return acc + got2[h, e - 1]

        totals[h, b] = lax.fori_loop(1, nb, add_sum, sums[h, b])
        loop(1, nb, lambda e: copy3(h, e).start())

    def add_part(e, acc):
        part_copy(e).wait_recv()
        return acc + parts[e - 1]

    counts = lax.fori_loop(1, nb, add_part, part[...])
    scale = 1.0 / (LR * counts)

    def copy4(h, d):
        target = out.at[pl.ds(own, share), pl.ds(h * LANES, LANES)]
        return remote(picked.at[h, d - 1], target, send4.at[h], recv4.at[h, d - 1], behind(d))

    for h in range(chunks):
        loop(1, nb, lambda e: copy3(h, e).wait_recv())
        means = [totals[h, k] * scale[k : k + 1, :] for k in range(CLUSTERS)]

        def choose(tile):
            value = jnp.zeros_like(means[0])
            for k in range(CLUSTERS):
                value = jnp.where(tile[k : k + 1, :] > 0.0, means[k], value)
            return value

        def give(d):
            picked[h, d - 1] = choose(meta[d - 1])
            copy4(h, d).start()

        loop(1, plane, give)
        out[pl.ds(own, share), pl.ds(h * LANES, LANES)] = choose(mine[...])

    for h in range(chunks):
        loop(1, plane, lambda d: copy4(h, d).wait_recv())

    loop(1, plane, lambda d: meta_copy(d, ahead(d)).wait_send())
    loop(1, nb, lambda e: part_copy(e).wait_send())
    for h in range(chunks):
        loop(1, plane, lambda d: copy1(h, d).wait_send())
        loop(1, nb, lambda e: copy2(h, e).wait_send())
        loop(1, nb, lambda e: copy3(h, e).wait_send())
        loop(1, plane, lambda d: copy4(h, d).wait_send())


def on_device(sizes, features, targets, lower_weight, head_weight, batch_rows, sample_counts, cluster_ids):
    nc, nb, nx = sizes
    plane = nc * nx
    _, pool, inside = features.shape
    _, hid, outs = head_weight.shape
    steps = batch_rows.shape[1]
    chunks = outs // LANES
    share = hid // plane
    blocks = pool // min(BLOCK, pool)
    hbm = pl.BlockSpec(memory_space=pltpu.HBM)
    vmem = pl.BlockSpec(memory_space=pltpu.VMEM)
    smem = pl.BlockSpec(memory_space=pltpu.SMEM)
    dma = pltpu.SemaphoreType.DMA
    f32, bf16 = jnp.float32, jnp.bfloat16
    result = pl.pallas_call(
        functools.partial(kernel, sizes),
        out_shape=jax.ShapeDtypeStruct((hid, outs), f32),
        in_specs=[hbm, hbm, hbm, hbm, vmem, smem, smem],
        out_specs=vmem,
        scratch_shapes=[
            pltpu.VMEM((pool, inside), bf16),
            pltpu.VMEM((pool, outs), bf16),
            pltpu.VMEM((inside, hid), bf16),
            pltpu.VMEM((hid, outs), f32),
            pltpu.VMEM((pool, hid), bf16),
            pltpu.VMEM((pool, hid), bf16),
            pltpu.VMEM((pool, outs), bf16),
            pltpu.VMEM((pool, outs), bf16),
            pltpu.VMEM((steps, LANES, pool // LANES), f32),
            pltpu.VMEM((chunks, hid, LANES), f32),
            pltpu.VMEM((CLUSTERS, LANES), f32),
            pltpu.VMEM((plane - 1, CLUSTERS, LANES), f32),
            pltpu.VMEM((CLUSTERS, LANES), f32),
            pltpu.VMEM((nb - 1, CLUSTERS, LANES), f32),
            pltpu.VMEM((chunks, plane - 1, share, LANES), f32),
            pltpu.VMEM((chunks, CLUSTERS, share, LANES), f32),
            pltpu.VMEM((chunks, nb - 1, share, LANES), f32),
            pltpu.VMEM((chunks, CLUSTERS, share, LANES), f32),
            pltpu.VMEM((chunks, plane - 1, share, LANES), f32),
            dma((blocks + 3,)),
            dma, dma((plane - 1,)), dma, dma((nb - 1,)),
            dma((chunks,)), dma((chunks, plane - 1)),
            dma((chunks,)), dma((chunks, nb - 1)),
            dma((chunks,)), dma((chunks, nb - 1)),
            dma((chunks,)), dma((chunks, plane - 1)),
        ],
        compiler_params=pltpu.CompilerParams(
            collective_id=0, has_side_effects=True, vmem_limit_bytes=64000 * 1024
        ),
    )(features, targets, lower_weight, head_weight, batch_rows, sample_counts, cluster_ids)
    return result[None]


def solution(mesh):
    sizes = tuple(mesh.shape[a] for a in AXES)
    whole = P(AXES)
    matrix = P(AXES, None, None)
    return jax.shard_map(
        functools.partial(on_device, sizes),
        mesh=mesh,
        in_specs=(matrix, matrix, matrix, matrix, matrix, whole, whole),
        out_specs=matrix,
        check_vma=False,
    )
```

```python
import functools
import math

import jax
import jax.numpy as jnp
from jax import lax
from jax.experimental import pallas as pl
from jax.experimental.pallas import tpu as pltpu
from jax.sharding import PartitionSpec as P

AXES = ("chip", "board", "cuts")
LR = 0.5
CLUSTERS = 8
LANES = 128
BLOCK = 512
PIECE = 256
SUBLANES = 8
SPLIT_COLUMNS = False
GRANT = 64000 * 1024
MESH = pl.DeviceIdType.MESH
NN = (((1,), (0,)), ((), ()))
NT = (((1,), (1,)), ((), ()))
TN = (((0,), (0,)), ((), ()))


def product(a, b, dims):
    return lax.dot_general(a, b, dims, preferred_element_type=jnp.float32)


def split(value):
    high = value.astype(jnp.bfloat16)
    return high, (value - high.astype(jnp.float32)).astype(jnp.bfloat16)


def load_all(pairs, sems):
    copies = [pltpu.make_async_copy(src, dst, sems.at[k]) for k, (src, dst) in enumerate(pairs)]
    for copy in copies:
        copy.start()
    return copies


def count_draws(rows, m_ref):
    steps, drawn = rows.shape
    for step in range(steps):
        index = rows[pl.ds(step, 1), :]
        inner = lax.broadcasted_iota(jnp.int32, (LANES, drawn), 0) == index % LANES
        outer = lax.broadcasted_iota(jnp.int32, (m_ref.shape[2], drawn), 0) == index // LANES
        m_ref[step] = product(
            inner.astype(jnp.float32).astype(jnp.bfloat16),
            outer.astype(jnp.float32).astype(jnp.bfloat16),
            NT,
        )


def errors(step, weight, columns, m_ref, t_ref, hh_ref, hl_ref, e_ref):
    wh, wl = split(weight)
    wide = weight.shape[1]
    pool = hh_ref.shape[0]
    piece = min(PIECE, pool)
    per = piece // LANES
    for k in range(pool // piece):
        rows = pl.ds(k * piece, piece)
        high, low = hh_ref[rows], hl_ref[rows]
        if wide == LANES:
            both = product(high, jnp.concatenate([wh, wl], 1), NN)
            err = both[:, :wide] + both[:, wide:] + product(low, wh, NN)
        else:
            err = product(high, wh, NN) + product(low, wh, NN) + product(high, wl, NN)
        err = err - t_ref[rows, columns].astype(jnp.float32)
        err = jnp.concatenate(
            [
                err[q * LANES : (q + 1) * LANES] * m_ref[step, :, pl.ds(k * per + q, 1)]
                for q in range(per)
            ],
            0,
        )
        e_ref[rows, :wide], e_ref[rows, wide : 2 * wide] = split(err)


def gradient(wide, rows, hh_ref, hl_ref, e_ref):
    high = hh_ref[:, rows]
    if wide == LANES:
        both = product(e_ref[:, : 2 * wide], high, TN)
        grad = both[:wide] + both[wide:] + product(e_ref[:, :wide], hl_ref[:, rows], TN)
    else:
        grad = product(e_ref[:, :wide], high, TN) + product(e_ref[:, :wide], hl_ref[:, rows], TN)
        grad = grad + product(e_ref[:, wide : 2 * wide], high, TN)
    return grad.T


def kernel(
    sizes,
    features, targets, lower, head, rows, count, cluster,
    out,
    x_ref, t_ref, v_ref, w_ref, hh_ref, hl_ref, e_ref, m_ref, rows_ref, count_ref, cluster_ref,
    delta, mine, meta, part, parts, got1, sums, got2, totals, picked,
    load_sems, meta_send, meta_recv, part_send, part_recv,
    send1, recv1, send2, recv2, send3, recv3, send4, recv4,
):
    nc, nb, nx = sizes
    plane = nc * nx
    chunks = delta.shape[0]
    share = SUBLANES
    hid, outs = w_ref.shape
    half = share * plane
    c, b, x = (lax.axis_index(a) for a in AXES)
    own = pl.multiple_of((c * nx + x) * share, share)

    def ahead(d):
        return (lax.rem(c + d // nx, nc), b, lax.rem(x + lax.rem(d, nx), nx))

    def behind(d):
        return (lax.rem(c + nc - d // nx, nc), b, lax.rem(x + nx - lax.rem(d, nx), nx))

    def along(e):
        return (c, lax.rem(b + e, nb), x)

    def steps_of(d, n):
        return min(d, n - d)

    order = sorted(
        range(1, plane),
        key=lambda d: -steps_of(d // nx // 2, max(nc // 2, 1)) - steps_of(d % nx, nx),
    )

    def remote(src, dst, send, recv, device):
        return pltpu.make_async_remote_copy(
            src_ref=src, dst_ref=dst, send_sem=send, recv_sem=recv, device_id=device, device_id_type=MESH
        )

    def loop(lo, hi, body):
        def run(k, carry):
            body(k)
            return carry

        lax.fori_loop(lo, hi, run, 0)

    def done(ref, sem):
        pltpu.make_async_copy(ref, ref, sem).wait()

    block = min(BLOCK, x_ref.shape[0])
    blocks = x_ref.shape[0] // block
    pairs = [(rows.at[0], rows_ref), (lower.at[0], v_ref)]
    for k in range(blocks):
        pairs.append((features.at[0, pl.ds(k * block, block)], x_ref.at[pl.ds(k * block, block)]))
    pairs += [(head.at[0], w_ref), (targets.at[0], t_ref), (count, count_ref), (cluster, cluster_ref)]
    copies = load_all(pairs, load_sems)
    barrier = pltpu.get_barrier_semaphore()
    loop(1, plane, lambda d: pl.semaphore_signal(barrier, inc=1, device_id=ahead(d), device_id_type=MESH))
    loop(1, nb, lambda e: pl.semaphore_signal(barrier, inc=1, device_id=along(e), device_id_type=MESH))
    copies[0].wait()
    count_draws(rows_ref, m_ref)
    copies[1].wait()
    for k in range(blocks):
        copies[2 + k].wait()
        here = pl.ds(k * block, block)
        hh_ref[here], hl_ref[here] = split(jnp.tanh(product(x_ref[here], v_ref[...], NN)))
    for copy in copies[2 + blocks :]:
        copy.wait()

    place = lax.broadcasted_iota(jnp.int32, mine.shape, 0) == cluster_ref[0]
    mine[...] = jnp.where(place, count_ref[0].astype(jnp.float32), 0.0)

    def meta_copy(d):
        return remote(mine, meta.at[d - 1], meta_send, meta_recv, ahead(d))

    def copy1(h, d):
        peer = ahead(d)
        at = pl.multiple_of((peer[0] * nx + peer[2]) * share, share)
        return remote(delta.at[h, pl.ds(at, share)], got1.at[h, d - 1], send1.at[h], recv1.at[h], peer)

    drawn = rows_ref.shape[1]
    rate = -LR / drawn
    wide = LANES if SPLIT_COLUMNS else outs
    tiles = wide // LANES
    h = 0
    places = []
    for col in range(0, outs, wide):
        columns = slice(col, col + wide)
        start = w_ref[:, columns]
        errors(0, start, columns, m_ref, t_ref, hh_ref, hl_ref, e_ref)
        first = gradient(wide, slice(None), hh_ref, hl_ref, e_ref) * rate
        if col == 0:
            pl.semaphore_wait(barrier, plane - 1 + nb - 1)
            loop(1, plane, lambda d: meta_copy(d).start())
        errors(1, start + first, columns, m_ref, t_ref, hh_ref, hl_ref, e_ref)
        for row in range(0, hid, half):
            change = first[row : row + half] + gradient(wide, slice(row, row + half), hh_ref, hl_ref, e_ref) * rate
            for t in range(tiles):
                delta[h] = change[:, t * LANES : (t + 1) * LANES]
                places.append((row, col + t * LANES))
                for d in order:
                    copy1(h, d).start()
                h += 1

    done(meta, meta_recv)
    part[...] = mine[...] + jnp.sum(meta[...], axis=0)

    def part_copy(e):
        return remote(part, parts.at[e - 1], part_send, part_recv, along(e))

    loop(1, nb, lambda e: part_copy(e).start())

    def copy2(h, e):
        peer = along(e)
        return remote(sums.at[h, peer[1]], got2.at[h, e - 1], send2.at[h], recv2.at[h], peer)

    def copy3(h, e):
        return remote(totals.at[h, b], totals.at[h, b], send3.at[h], recv3.at[h], along(e))

    def target(h):
        row, col = places[h]
        return out.at[pl.ds(row + own, share), pl.ds(col, LANES)]

    def copy4(h, d):
        return remote(picked.at[h, d - 1], target(h), send4.at[h], recv4.at[h], behind(d))

    def stage1(h):
        done(got1.at[h], recv1.at[h])
        value = delta[h, pl.ds(own, share)]
        got = got1[h]
        for k in range(CLUSTERS):
            sums[h, k] = value * mine[pl.ds(k, 1), :] + jnp.sum(got * meta[:, k : k + 1, :], axis=0)
        loop(1, nb, lambda e: copy2(h, e).start())

    def stage2(h):
        done(got2.at[h], recv2.at[h])
        totals[h, b] = sums[h, b] + jnp.sum(got2[h], axis=0)
        loop(1, nb, lambda e: copy3(h, e).start())

    def stage3(h, scale):
        done(got2.at[h], recv3.at[h])
        value = jnp.zeros(picked.shape[1:], jnp.float32)
        kept = jnp.zeros((share, LANES), jnp.float32)
        for k in range(CLUSTERS):
            mean = totals[h, k] * scale[k : k + 1, :]
            value = jnp.where(meta[:, k : k + 1, :] > 0.0, mean[None], value)
            kept = jnp.where(mine[pl.ds(k, 1), :] > 0.0, mean, kept)
        picked[h] = value
        for d in order:
            copy4(h, d).start()
        row, col = places[h]
        out[pl.ds(row + own, share), pl.ds(col, LANES)] = kept

    for h in range(chunks):
        stage1(h)
    for h in range(chunks):
        stage2(h)
    done(parts, part_recv)
    scale = 1.0 / (LR * (part[...] + jnp.sum(parts[...], axis=0)))
    for h in range(chunks):
        stage3(h, scale)
    for h in range(chunks):
        done(got1.at[h], recv4.at[h])

    done(meta, meta_send)
    done(parts, part_send)
    for h in range(chunks):
        done(got1.at[h], send1.at[h])
        done(got2.at[h], send2.at[h])
        done(got2.at[h], send3.at[h])
        done(got1.at[h], send4.at[h])


def on_device(sizes, features, targets, lower_weight, head_weight, batch_rows, sample_counts, cluster_ids):
    nc, nb, nx = sizes
    plane = nc * nx
    _, pool, inside = features.shape
    _, hid, outs = head_weight.shape
    _, steps, drawn = batch_rows.shape
    share = SUBLANES
    chunks = hid // (plane * share) * (outs // LANES)
    blocks = pool // min(BLOCK, pool)
    hbm = pl.BlockSpec(memory_space=pltpu.HBM)
    vmem = pl.BlockSpec(memory_space=pltpu.VMEM)
    dma = pltpu.SemaphoreType.DMA
    f32, bf16 = jnp.float32, jnp.bfloat16
    result = pl.pallas_call(
        functools.partial(kernel, sizes),
        out_shape=jax.ShapeDtypeStruct((hid, outs), f32),
        in_specs=[hbm] * 7,
        out_specs=vmem,
        scratch_shapes=[
            pltpu.VMEM((pool, inside), bf16),
            pltpu.VMEM((pool, outs), bf16),
            pltpu.VMEM((inside, hid), bf16),
            pltpu.VMEM((hid, outs), f32),
            pltpu.VMEM((pool, hid), bf16),
            pltpu.VMEM((pool, hid), bf16),
            pltpu.VMEM((pool, 2 * outs), bf16),
            pltpu.VMEM((steps, LANES, pool // LANES), f32),
            pltpu.VMEM((steps, drawn), jnp.int32),
            pltpu.SMEM((1,), jnp.int32),
            pltpu.SMEM((1,), jnp.int32),
            pltpu.VMEM((chunks, plane * share, LANES), f32),
            pltpu.VMEM((CLUSTERS, LANES), f32),
            pltpu.VMEM((plane - 1, CLUSTERS, LANES), f32),
            pltpu.VMEM((CLUSTERS, LANES), f32),
            pltpu.VMEM((nb - 1, CLUSTERS, LANES), f32),
            pltpu.VMEM((chunks, plane - 1, share, LANES), f32),
            pltpu.VMEM((chunks, CLUSTERS, share, LANES), f32),
            pltpu.VMEM((chunks, nb - 1, share, LANES), f32),
            pltpu.VMEM((chunks, CLUSTERS, share, LANES), f32),
            pltpu.VMEM((chunks, plane - 1, share, LANES), f32),
            dma((blocks + 6,)),
            dma, dma, dma, dma,
            *[dma((chunks,)) for _ in range(8)],
        ],
        compiler_params=pltpu.CompilerParams(
            collective_id=0, has_side_effects=True, vmem_limit_bytes=GRANT
        ),
    )(features, targets, lower_weight, head_weight, batch_rows, sample_counts, cluster_ids)
    return result[None]


def solution(mesh):
    sizes = tuple(mesh.shape[a] for a in AXES)
    whole = P(AXES)
    matrix = P(AXES, None, None)
    return jax.shard_map(
        functools.partial(on_device, sizes),
        mesh=mesh,
        in_specs=(matrix, matrix, matrix, matrix, matrix, whole, whole),
        out_specs=matrix,
        check_vma=False,
    )
```

```python
import functools
import math

import jax
import jax.numpy as jnp
from jax import lax
from jax.experimental import pallas as pl
from jax.experimental.pallas import tpu as pltpu
from jax.sharding import PartitionSpec as P

AXES = ("chip", "board", "cuts")
LR = 0.5
CLUSTERS = 8
LANES = 128
BLOCK = 512
PIECE = 256
SUBLANES = 8
SPLIT_COLUMNS = False
GRANT = 48000 * 1024
MESH = pl.DeviceIdType.MESH
NN = (((1,), (0,)), ((), ()))
NT = (((1,), (1,)), ((), ()))
TN = (((0,), (0,)), ((), ()))


def product(a, b, dims):
    return lax.dot_general(a, b, dims, preferred_element_type=jnp.float32)


def split(value):
    high = value.astype(jnp.bfloat16)
    return high, (value - high.astype(jnp.float32)).astype(jnp.bfloat16)


def load_all(pairs, sems):
    copies = [pltpu.make_async_copy(src, dst, sems.at[k]) for k, (src, dst) in enumerate(pairs)]
    for copy in copies:
        copy.start()
    return copies


def count_draws(rows, m_ref):
    steps, drawn = rows.shape
    for step in range(steps):
        index = rows[pl.ds(step, 1), :]
        inner = lax.broadcasted_iota(jnp.int32, (LANES, drawn), 0) == index % LANES
        outer = lax.broadcasted_iota(jnp.int32, (m_ref.shape[2], drawn), 0) == index // LANES
        m_ref[step] = product(
            inner.astype(jnp.float32).astype(jnp.bfloat16),
            outer.astype(jnp.float32).astype(jnp.bfloat16),
            NT,
        )


def errors(step, weight, columns, m_ref, t_ref, hh_ref, hl_ref, e_ref):
    wh, wl = split(weight)
    wide = weight.shape[1]
    pool = hh_ref.shape[0]
    piece = min(PIECE, pool)
    per = piece // LANES
    for k in range(pool // piece):
        rows = pl.ds(k * piece, piece)
        high, low = hh_ref[rows], hl_ref[rows]
        if wide == LANES:
            both = product(high, jnp.concatenate([wh, wl], 1), NN)
            err = both[:, :wide] + both[:, wide:] + product(low, wh, NN)
        else:
            err = product(high, wh, NN) + product(low, wh, NN) + product(high, wl, NN)
        err = err - t_ref[rows, columns].astype(jnp.float32)
        err = jnp.concatenate(
            [
                err[q * LANES : (q + 1) * LANES] * m_ref[step, :, pl.ds(k * per + q, 1)]
                for q in range(per)
            ],
            0,
        )
        e_ref[rows, :wide], e_ref[rows, wide : 2 * wide] = split(err)


def gradient(wide, rows, hh_ref, hl_ref, e_ref):
    high = hh_ref[:, rows]
    if wide == LANES:
        both = product(e_ref[:, : 2 * wide], high, TN)
        grad = both[:wide] + both[wide:] + product(e_ref[:, :wide], hl_ref[:, rows], TN)
    else:
        grad = product(e_ref[:, :wide], high, TN) + product(e_ref[:, :wide], hl_ref[:, rows], TN)
        grad = grad + product(e_ref[:, wide : 2 * wide], high, TN)
    return grad.T


def kernel(
    sizes,
    features, targets, lower, head, rows, mine,
    out,
    x_ref, t_ref, v_ref, w_ref, hh_ref, hl_ref, e_ref, m_ref, rows_ref,
    delta, meta, part, parts, got1, sums, got2, totals, picked,
    load_sems, meta_send, meta_recv, part_send, part_recv,
    send1, recv1, send2, recv2, send3, recv3, send4, recv4,
):
    nc, nb, nx = sizes
    plane = nc * nx
    chunks = delta.shape[0]
    share = SUBLANES
    hid, outs = w_ref.shape
    half = share * plane
    c, b, x = (lax.axis_index(a) for a in AXES)
    own = pl.multiple_of((c * nx + x) * share, share)

    def ahead(d):
        return (lax.rem(c + d // nx, nc), b, lax.rem(x + lax.rem(d, nx), nx))

    def behind(d):
        return (lax.rem(c + nc - d // nx, nc), b, lax.rem(x + nx - lax.rem(d, nx), nx))

    def along(e):
        return (c, lax.rem(b + e, nb), x)

    def steps_of(d, n):
        return min(d, n - d)

    order = sorted(
        range(1, plane),
        key=lambda d: -steps_of(d // nx // 2, max(nc // 2, 1)) - steps_of(d % nx, nx),
    )

    def remote(src, dst, send, recv, device):
        return pltpu.make_async_remote_copy(
            src_ref=src, dst_ref=dst, send_sem=send, recv_sem=recv, device_id=device, device_id_type=MESH
        )

    def loop(lo, hi, body):
        def run(k, carry):
            body(k)
            return carry

        lax.fori_loop(lo, hi, run, 0)

    def done(ref, sem):
        pltpu.make_async_copy(ref, ref, sem).wait()

    block = min(BLOCK, x_ref.shape[0])
    blocks = x_ref.shape[0] // block
    pairs = [(rows.at[0], rows_ref), (lower.at[0], v_ref)]
    for k in range(blocks):
        pairs.append((features.at[0, pl.ds(k * block, block)], x_ref.at[pl.ds(k * block, block)]))
    pairs += [(head.at[0], w_ref), (targets.at[0], t_ref)]
    copies = load_all(pairs, load_sems)
    barrier = pltpu.get_barrier_semaphore()
    loop(1, plane, lambda d: pl.semaphore_signal(barrier, inc=1, device_id=ahead(d), device_id_type=MESH))
    loop(1, nb, lambda e: pl.semaphore_signal(barrier, inc=1, device_id=along(e), device_id_type=MESH))
    copies[0].wait()
    count_draws(rows_ref, m_ref)
    copies[1].wait()
    for k in range(blocks):
        copies[2 + k].wait()
        if k == blocks - 1:
            for copy in copies[2 + blocks :]:
                copy.wait()
        here = pl.ds(k * block, block)
        hh_ref[here], hl_ref[here] = split(jnp.tanh(product(x_ref[here], v_ref[...], NN)))

    def meta_copy(d):
        return remote(mine, meta.at[d - 1], meta_send, meta_recv, ahead(d))

    def copy1(h, d):
        peer = ahead(d)
        at = pl.multiple_of((peer[0] * nx + peer[2]) * share, share)
        return remote(delta.at[h, pl.ds(at, share)], got1.at[h, d - 1], send1.at[h], recv1.at[h], peer)

    drawn = rows_ref.shape[1]
    rate = -LR / drawn
    wide = LANES if SPLIT_COLUMNS else outs
    tiles = wide // LANES
    h = 0
    places = []
    for col in range(0, outs, wide):
        columns = slice(col, col + wide)
        start = w_ref[:, columns]
        errors(0, start, columns, m_ref, t_ref, hh_ref, hl_ref, e_ref)
        first = gradient(wide, slice(None), hh_ref, hl_ref, e_ref) * rate
        if col == 0:
            pl.semaphore_wait(barrier, plane - 1 + nb - 1)
            loop(1, plane, lambda d: meta_copy(d).start())
        errors(1, start + first, columns, m_ref, t_ref, hh_ref, hl_ref, e_ref)
        for row in range(0, hid, half):
            change = first[row : row + half] + gradient(wide, slice(row, row + half), hh_ref, hl_ref, e_ref) * rate
            for t in range(tiles):
                delta[h] = change[:, t * LANES : (t + 1) * LANES]
                places.append((row, col + t * LANES))
                for d in order:
                    copy1(h, d).start()
                h += 1

    done(meta, meta_recv)
    part[...] = mine[...] + jnp.sum(meta[...], axis=0)

    def part_copy(e):
        return remote(part, parts.at[e - 1], part_send, part_recv, along(e))

    loop(1, nb, lambda e: part_copy(e).start())

    def copy2(h, e):
        peer = along(e)
        return remote(sums.at[h, peer[1]], got2.at[h, e - 1], send2.at[h], recv2.at[h], peer)

    def copy3(h, e):
        return remote(totals.at[h, b], totals.at[h, b], send3.at[h], recv3.at[h], along(e))

    def target(h):
        row, col = places[h]
        return out.at[pl.ds(row + own, share), pl.ds(col, LANES)]

    def copy4(h, d):
        return remote(picked.at[h, d - 1], target(h), send4.at[h], recv4.at[h], behind(d))

    def stage1(h):
        done(got1.at[h], recv1.at[h])
        value = delta[h, pl.ds(own, share)]
        got = got1[h]
        for k in range(CLUSTERS):
            sums[h, k] = value * mine[pl.ds(k, 1), :] + jnp.sum(got * meta[:, k : k + 1, :], axis=0)
        loop(1, nb, lambda e: copy2(h, e).start())

    def stage2(h):
        done(got2.at[h], recv2.at[h])
        totals[h, b] = sums[h, b] + jnp.sum(got2[h], axis=0)
        loop(1, nb, lambda e: copy3(h, e).start())

    def stage3(h, scale):
        done(got2.at[h], recv3.at[h])
        value = jnp.zeros(picked.shape[1:], jnp.float32)
        kept = jnp.zeros((share, LANES), jnp.float32)
        for k in range(CLUSTERS):
            mean = totals[h, k] * scale[k : k + 1, :]
            value = jnp.where(meta[:, k : k + 1, :] > 0.0, mean[None], value)
            kept = jnp.where(mine[pl.ds(k, 1), :] > 0.0, mean, kept)
        picked[h] = value
        for d in order:
            copy4(h, d).start()
        row, col = places[h]
        out[pl.ds(row + own, share), pl.ds(col, LANES)] = kept

    for h in range(chunks):
        stage1(h)
    for h in range(chunks):
        stage2(h)
    done(parts, part_recv)
    scale = 1.0 / (LR * (part[...] + jnp.sum(parts[...], axis=0)))
    for h in range(chunks):
        stage3(h, scale)
    for h in range(chunks):
        done(got1.at[h], recv4.at[h])

    done(meta, meta_send)
    done(parts, part_send)
    for h in range(chunks):
        done(got1.at[h], send1.at[h])
        done(got2.at[h], send2.at[h])
        done(got2.at[h], send3.at[h])
        done(got1.at[h], send4.at[h])


def on_device(sizes, features, targets, lower_weight, head_weight, batch_rows, sample_counts, cluster_ids):
    nc, nb, nx = sizes
    plane = nc * nx
    _, pool, inside = features.shape
    _, hid, outs = head_weight.shape
    _, steps, drawn = batch_rows.shape
    share = SUBLANES
    chunks = hid // (plane * share) * (outs // LANES)
    blocks = pool // min(BLOCK, pool)
    hbm = pl.BlockSpec(memory_space=pltpu.HBM)
    vmem = pl.BlockSpec(memory_space=pltpu.VMEM)
    dma = pltpu.SemaphoreType.DMA
    f32, bf16 = jnp.float32, jnp.bfloat16
    place = lax.broadcasted_iota(jnp.int32, (CLUSTERS, LANES), 0) == cluster_ids[0]
    mine = jnp.where(place, sample_counts[0].astype(f32), 0.0)
    held = [
        pltpu.with_memory_space_constraint(v, pltpu.HBM)
        for v in (features, targets, lower_weight, head_weight, batch_rows)
    ]
    result = pl.pallas_call(
        functools.partial(kernel, sizes),
        out_shape=jax.ShapeDtypeStruct((hid, outs), f32),
        in_specs=[hbm] * 5 + [vmem],
        out_specs=vmem,
        scratch_shapes=[
            pltpu.VMEM((pool, inside), bf16),
            pltpu.VMEM((pool, outs), bf16),
            pltpu.VMEM((inside, hid), bf16),
            pltpu.VMEM((hid, outs), f32),
            pltpu.VMEM((pool, hid), bf16),
            pltpu.VMEM((pool, hid), bf16),
            pltpu.VMEM((pool, 2 * outs), bf16),
            pltpu.VMEM((steps, LANES, pool // LANES), f32),
            pltpu.VMEM((steps, drawn), jnp.int32),
            pltpu.VMEM((chunks, plane * share, LANES), f32),
            pltpu.VMEM((plane - 1, CLUSTERS, LANES), f32),
            pltpu.VMEM((CLUSTERS, LANES), f32),
            pltpu.VMEM((nb - 1, CLUSTERS, LANES), f32),
            pltpu.VMEM((chunks, plane - 1, share, LANES), f32),
            pltpu.VMEM((chunks, CLUSTERS, share, LANES), f32),
            pltpu.VMEM((chunks, nb - 1, share, LANES), f32),
            pltpu.VMEM((chunks, CLUSTERS, share, LANES), f32),
            pltpu.VMEM((chunks, plane - 1, share, LANES), f32),
            dma((blocks + 4,)),
            dma, dma, dma, dma,
            *[dma((chunks,)) for _ in range(8)],
        ],
        compiler_params=pltpu.CompilerParams(
            collective_id=0, has_side_effects=True, vmem_limit_bytes=GRANT
        ),
    )(*held, mine)
    return result[None]


def solution(mesh):
    sizes = tuple(mesh.shape[a] for a in AXES)
    whole = P(AXES)
    matrix = P(AXES, None, None)
    return jax.shard_map(
        functools.partial(on_device, sizes),
        mesh=mesh,
        in_specs=(matrix, matrix, matrix, matrix, matrix, whole, whole),
        out_specs=matrix,
        check_vma=False,
    )
```

```python
import functools
import math

import jax
import jax.numpy as jnp
from jax import lax
from jax.experimental import pallas as pl
from jax.experimental.pallas import tpu as pltpu
from jax.sharding import PartitionSpec as P

AXES = ("chip", "board", "cuts")
LR = 0.5
CLUSTERS = 8
LANES = 128
BLOCK = 512
PIECE = 512
SUBLANES = 8
WIDE = 128
GRANT = 48000 * 1024
MESH = pl.DeviceIdType.MESH
NN = (((1,), (0,)), ((), ()))
NT = (((1,), (1,)), ((), ()))
TN = (((0,), (0,)), ((), ()))


def product(a, b, dims):
    return lax.dot_general(a, b, dims, preferred_element_type=jnp.float32)


def split(value):
    high = value.astype(jnp.bfloat16)
    return high, (value - high.astype(jnp.float32)).astype(jnp.bfloat16)


def load_all(pairs, sems):
    copies = [pltpu.make_async_copy(src, dst, sems.at[k]) for k, (src, dst) in enumerate(pairs)]
    for copy in copies:
        copy.start()
    return copies


def count_draws(rows, m_ref):
    steps, drawn = rows.shape
    for step in range(steps):
        index = rows[pl.ds(step, 1), :]
        inner = lax.broadcasted_iota(jnp.int32, (LANES, drawn), 0) == index % LANES
        outer = lax.broadcasted_iota(jnp.int32, (m_ref.shape[1], drawn), 0) == index // LANES
        m_ref[step] = product(
            outer.astype(jnp.float32).astype(jnp.bfloat16),
            inner.astype(jnp.float32).astype(jnp.bfloat16),
            NT,
        )


def errors(step, weight, columns, m_ref, t_ref, hh_ref, hl_ref, e_ref):
    wh, wl = split(weight)
    outs = weight.shape[0]
    pool = hh_ref.shape[0]
    piece = min(PIECE, pool)
    per = piece // LANES
    for k in range(pool // piece):
        rows = pl.ds(k * piece, piece)
        high, low = hh_ref[rows], hl_ref[rows]
        if outs == LANES:
            err = product(high, jnp.concatenate([wh, wl], 0), NT)
            err = err[:, :outs] + err[:, outs:] + product(low, wh, NT)
        else:
            err = product(high, wh, NT) + product(low, wh, NT) + product(high, wl, NT)
        err = (err - t_ref[rows, columns].astype(jnp.float32)).T
        err = jnp.concatenate(
            [
                err[:, q * LANES : (q + 1) * LANES] * m_ref[step, pl.ds(k * per + q, 1), :]
                for q in range(per)
            ],
            1,
        )
        e_ref[:outs, rows], e_ref[outs : 2 * outs, rows] = split(err)


def gradient(outs, rows, hh_ref, hl_ref, e_ref):
    high = hh_ref[:, rows]
    if outs == LANES:
        grad = product(e_ref[: 2 * outs], high, NN)
        return grad[:outs] + grad[outs:] + product(e_ref[:outs], hl_ref[:, rows], NN)
    grad = product(e_ref[:outs], high, NN) + product(e_ref[:outs], hl_ref[:, rows], NN)
    return grad + product(e_ref[outs : 2 * outs], high, NN)


def kernel(
    sizes,
    features, targets, lower, head, rows, mine,
    out,
    x_ref, t_ref, v_ref, w_ref, hh_ref, hl_ref, e_ref, m_ref, rows_ref,
    delta, meta, part, parts, got1, sums, got2, totals, picked,
    load_sems, meta_send, meta_recv, part_send, part_recv,
    send1, recv1, send2, recv2, send3, recv3, send4, recv4,
):
    nc, nb, nx = sizes
    plane = nc * nx
    chunks = delta.shape[0]
    share = SUBLANES
    hid, outs = w_ref.shape
    half = share * plane
    c, b, x = (lax.axis_index(a) for a in AXES)
    own = pl.multiple_of((c * nx + x) * share, share)

    def ahead(d):
        return (lax.rem(c + d // nx, nc), b, lax.rem(x + lax.rem(d, nx), nx))

    def behind(d):
        return (lax.rem(c + nc - d // nx, nc), b, lax.rem(x + nx - lax.rem(d, nx), nx))

    def along(e):
        return (c, lax.rem(b + e, nb), x)

    def steps_of(d, n):
        return min(d, n - d)

    order = sorted(
        range(1, plane),
        key=lambda d: -steps_of(d // nx // 2, max(nc // 2, 1)) - steps_of(d % nx, nx),
    )

    z_order = sorted(range(1, nb), key=lambda e: -steps_of(e, nb))

    def remote(src, dst, send, recv, device):
        return pltpu.make_async_remote_copy(
            src_ref=src, dst_ref=dst, send_sem=send, recv_sem=recv, device_id=device, device_id_type=MESH
        )

    def loop(lo, hi, body):
        def run(k, carry):
            body(k)
            return carry

        lax.fori_loop(lo, hi, run, 0)

    def done(ref, sem):
        pltpu.make_async_copy(ref, ref, sem).wait()

    def spread(value):
        return jnp.concatenate([value] * (WIDE // LANES), axis=-1)

    block = min(BLOCK, x_ref.shape[0])
    blocks = x_ref.shape[0] // block
    pairs = [(rows.at[0], rows_ref), (lower.at[0], v_ref)]
    for k in range(blocks):
        pairs.append((features.at[0, pl.ds(k * block, block)], x_ref.at[pl.ds(k * block, block)]))
    pairs += [(head.at[0], w_ref), (targets.at[0], t_ref)]
    copies = load_all(pairs, load_sems)
    barrier = pltpu.get_barrier_semaphore()
    loop(1, plane, lambda d: pl.semaphore_signal(barrier, inc=1, device_id=ahead(d), device_id_type=MESH))
    loop(1, nb, lambda e: pl.semaphore_signal(barrier, inc=1, device_id=along(e), device_id_type=MESH))
    copies[0].wait()
    count_draws(rows_ref, m_ref)
    copies[1].wait()
    for k in range(blocks):
        copies[2 + k].wait()
        if k == blocks - 1:
            for copy in copies[2 + blocks :]:
                copy.wait()
        here = pl.ds(k * block, block)
        hh_ref[here], hl_ref[here] = split(jnp.tanh(product(x_ref[here], v_ref[...], NN)))

    def meta_copy(d):
        return remote(mine, meta.at[d - 1], meta_send, meta_recv, ahead(d))

    def copy1(h, d):
        peer = ahead(d)
        at = pl.multiple_of((peer[0] * nx + peer[2]) * share, share)
        return remote(delta.at[h, pl.ds(at, share)], got1.at[h, d - 1], send1.at[h], recv1.at[h], peer)

    drawn = rows_ref.shape[1]
    rate = -LR / drawn
    h = 0
    places = []
    start = w_ref[...].T
    errors(0, start, slice(0, outs), m_ref, t_ref, hh_ref, hl_ref, e_ref)
    first = gradient(outs, slice(None), hh_ref, hl_ref, e_ref) * rate
    pl.semaphore_wait(barrier, plane - 1 + nb - 1)
    loop(1, plane, lambda d: meta_copy(d).start())
    for col in range(0, outs, WIDE):
        columns = slice(col, col + WIDE)
        errors(1, (start + first)[columns], columns, m_ref, t_ref, hh_ref, hl_ref, e_ref)
        for row in range(0, hid, half):
            change = gradient(WIDE, slice(row, row + half), hh_ref, hl_ref, e_ref) * rate
            delta[h] = (first[columns, row : row + half] + change).T
            places.append((row, col))
            for d in order:
                copy1(h, d).start()
            h += 1

    done(meta, meta_recv)
    part[...] = mine[...] + jnp.sum(meta[...], axis=0)

    def part_copy(e):
        return remote(part, parts.at[e - 1], part_send, part_recv, along(e))

    loop(1, nb, lambda e: part_copy(e).start())

    def copy2(h, e):
        peer = along(e)
        return remote(sums.at[h, peer[1]], got2.at[h, e - 1], send2.at[h], recv2.at[h], peer)

    def copy3(h, e):
        return remote(totals.at[h, b], totals.at[h, b], send3.at[h], recv3.at[h], along(e))

    def target(h):
        row, col = places[h]
        return out.at[pl.ds(row + own, share), pl.ds(col, WIDE)]

    def copy4(h, d):
        return remote(picked.at[h, d - 1], target(h), send4.at[h], recv4.at[h], behind(d))

    def stage1(h):
        done(got1.at[h], recv1.at[h])
        value = delta[h, pl.ds(own, share)]
        got = got1[h]
        for k in range(CLUSTERS):
            sums[h, k] = value * spread(mine[pl.ds(k, 1), :]) + jnp.sum(got * spread(meta[:, k : k + 1, :]), axis=0)
        for e in z_order:
            copy2(h, e).start()

    def stage2(h):
        done(got2.at[h], recv2.at[h])
        totals[h, b] = sums[h, b] + jnp.sum(got2[h], axis=0)
        for e in z_order:
            copy3(h, e).start()

    def stage3(h, scale):
        done(got2.at[h], recv3.at[h])
        value = jnp.zeros(picked.shape[1:], jnp.float32)
        kept = jnp.zeros((share, WIDE), jnp.float32)
        for k in range(CLUSTERS):
            mean = totals[h, k] * spread(scale[k : k + 1, :])
            value = jnp.where(spread(meta[:, k : k + 1, :]) > 0.0, mean[None], value)
            kept = jnp.where(spread(mine[pl.ds(k, 1), :]) > 0.0, mean, kept)
        picked[h] = value
        for d in order:
            copy4(h, d).start()
        row, col = places[h]
        out[pl.ds(row + own, share), pl.ds(col, WIDE)] = kept

    for h in range(chunks):
        stage1(h)
    for h in range(chunks):
        stage2(h)
    done(parts, part_recv)
    scale = 1.0 / (LR * (part[...] + jnp.sum(parts[...], axis=0)))
    for h in range(chunks):
        stage3(h, scale)
    for h in range(chunks):
        done(got1.at[h], recv4.at[h])

    done(meta, meta_send)
    done(parts, part_send)
    for h in range(chunks):
        done(got1.at[h], send1.at[h])
        done(got2.at[h], send2.at[h])
        done(got2.at[h], send3.at[h])
        done(got1.at[h], send4.at[h])


def on_device(sizes, features, targets, lower_weight, head_weight, batch_rows, sample_counts, cluster_ids):
    nc, nb, nx = sizes
    plane = nc * nx
    _, pool, inside = features.shape
    _, hid, outs = head_weight.shape
    _, steps, drawn = batch_rows.shape
    share = SUBLANES
    chunks = hid // (plane * share) * (outs // WIDE)
    blocks = pool // min(BLOCK, pool)
    hbm = pl.BlockSpec(memory_space=pltpu.HBM)
    vmem = pl.BlockSpec(memory_space=pltpu.VMEM)
    dma = pltpu.SemaphoreType.DMA
    f32, bf16 = jnp.float32, jnp.bfloat16
    place = lax.broadcasted_iota(jnp.int32, (CLUSTERS, LANES), 0) == cluster_ids[0]
    mine = jnp.where(place, sample_counts[0].astype(f32), 0.0)
    held = [
        pltpu.with_memory_space_constraint(v, pltpu.HBM)
        for v in (features, targets, lower_weight, head_weight, batch_rows)
    ]
    result = pl.pallas_call(
        functools.partial(kernel, sizes),
        out_shape=jax.ShapeDtypeStruct((hid, outs), f32),
        in_specs=[hbm] * 5 + [vmem],
        out_specs=vmem,
        scratch_shapes=[
            pltpu.VMEM((pool, inside), bf16),
            pltpu.VMEM((pool, outs), bf16),
            pltpu.VMEM((inside, hid), bf16),
            pltpu.VMEM((hid, outs), f32),
            pltpu.VMEM((pool, hid), bf16),
            pltpu.VMEM((pool, hid), bf16),
            pltpu.VMEM((2 * outs, pool), bf16),
            pltpu.VMEM((steps, pool // LANES, LANES), f32),
            pltpu.VMEM((steps, drawn), jnp.int32),
            pltpu.VMEM((chunks, plane * share, WIDE), f32),
            pltpu.VMEM((plane - 1, CLUSTERS, LANES), f32),
            pltpu.VMEM((CLUSTERS, LANES), f32),
            pltpu.VMEM((nb - 1, CLUSTERS, LANES), f32),
            pltpu.VMEM((chunks, plane - 1, share, WIDE), f32),
            pltpu.VMEM((chunks, CLUSTERS, share, WIDE), f32),
            pltpu.VMEM((chunks, nb - 1, share, WIDE), f32),
            pltpu.VMEM((chunks, CLUSTERS, share, WIDE), f32),
            pltpu.VMEM((chunks, plane - 1, share, WIDE), f32),
            dma((blocks + 4,)),
            dma, dma, dma, dma,
            *[dma((chunks,)) for _ in range(8)],
        ],
        compiler_params=pltpu.CompilerParams(
            collective_id=0, has_side_effects=True, vmem_limit_bytes=GRANT
        ),
    )(*held, mine)
    return result[None]


def solution(mesh):
    sizes = tuple(mesh.shape[a] for a in AXES)
    whole = P(AXES)
    matrix = P(AXES, None, None)
    return jax.shard_map(
        functools.partial(on_device, sizes),
        mesh=mesh,
        in_specs=(matrix, matrix, matrix, matrix, matrix, whole, whole),
        out_specs=matrix,
        check_vma=False,
    )
```

```python
import functools
import math

import jax
import jax.numpy as jnp
from jax import lax
from jax.experimental import pallas as pl
from jax.experimental.pallas import tpu as pltpu
from jax.sharding import PartitionSpec as P

AXES = ("chip", "board", "cuts")
LR = 0.5
CLUSTERS = 8
LANES = 128
BLOCK = 512
PIECE = 512
SUBLANES = 8
WIDE = 128
GRANT = 48000 * 1024
MESH = pl.DeviceIdType.MESH
NN = (((1,), (0,)), ((), ()))
NT = (((1,), (1,)), ((), ()))
TN = (((0,), (0,)), ((), ()))


def product(a, b, dims):
    return lax.dot_general(a, b, dims, preferred_element_type=jnp.float32)


def split(value):
    high = value.astype(jnp.bfloat16)
    return high, (value - high.astype(jnp.float32)).astype(jnp.bfloat16)


def load_all(pairs, sems):
    copies = [pltpu.make_async_copy(src, dst, sems.at[k]) for k, (src, dst) in enumerate(pairs)]
    for copy in copies:
        copy.start()
    return copies


def count_draws(rows, m_ref):
    steps, drawn = rows.shape
    for step in range(steps):
        index = rows[pl.ds(step, 1), :]
        inner = lax.broadcasted_iota(jnp.int32, (LANES, drawn), 0) == index % LANES
        outer = lax.broadcasted_iota(jnp.int32, (m_ref.shape[1], drawn), 0) == index // LANES
        m_ref[step] = product(
            outer.astype(jnp.float32).astype(jnp.bfloat16),
            inner.astype(jnp.float32).astype(jnp.bfloat16),
            NT,
        )


def errors(step, weight, columns, m_ref, t_ref, hh_ref, hl_ref, e_ref):
    wh, wl = split(weight)
    outs = weight.shape[0]
    pool = hh_ref.shape[0]
    piece = min(PIECE, pool)
    per = piece // LANES
    for k in range(pool // piece):
        rows = pl.ds(k * piece, piece)
        high, low = hh_ref[rows], hl_ref[rows]
        if outs == LANES:
            err = product(high, jnp.concatenate([wh, wl], 0), NT)
            err = err[:, :outs] + err[:, outs:] + product(low, wh, NT)
        else:
            err = product(high, wh, NT) + product(low, wh, NT) + product(high, wl, NT)
        err = (err - t_ref[rows, columns].astype(jnp.float32)).T
        err = jnp.concatenate(
            [
                err[:, q * LANES : (q + 1) * LANES] * m_ref[step, pl.ds(k * per + q, 1), :]
                for q in range(per)
            ],
            1,
        )
        e_ref[:outs, rows], e_ref[outs : 2 * outs, rows] = split(err)


def gradient(outs, rows, hh_ref, hl_ref, e_ref):
    high = hh_ref[:, rows]
    if outs == LANES:
        grad = product(e_ref[: 2 * outs], high, NN)
        return grad[:outs] + grad[outs:] + product(e_ref[:outs], hl_ref[:, rows], NN)
    grad = product(e_ref[:outs], high, NN) + product(e_ref[:outs], hl_ref[:, rows], NN)
    return grad + product(e_ref[outs : 2 * outs], high, NN)


def kernel(
    sizes,
    features, targets, lower, head, rows, mine,
    out,
    x_ref, t_ref, v_ref, w_ref, hh_ref, hl_ref, e_ref, m_ref, rows_ref,
    delta, meta, part, parts, got1, sums, got2, totals, picked,
    load_sems, meta_send, meta_recv, part_send, part_recv,
    send1, recv1, send2, recv2, send3, recv3, send4, recv4,
):
    nc, nb, nx = sizes
    plane = nc * nx
    chunks = delta.shape[0]
    share = SUBLANES
    hid, outs = w_ref.shape
    half = share * plane
    c, b, x = (lax.axis_index(a) for a in AXES)
    own = pl.multiple_of((c * nx + x) * share, share)

    def ahead(d):
        return (lax.rem(c + d // nx, nc), b, lax.rem(x + lax.rem(d, nx), nx))

    def behind(d):
        return (lax.rem(c + nc - d // nx, nc), b, lax.rem(x + nx - lax.rem(d, nx), nx))

    def along(e):
        return (c, lax.rem(b + e, nb), x)

    def steps_of(d, n):
        return min(d, n - d)

    order = sorted(
        range(1, plane),
        key=lambda d: -steps_of(d // nx // 2, max(nc // 2, 1)) - steps_of(d % nx, nx),
    )

    z_order = sorted(range(1, nb), key=lambda e: -steps_of(e, nb))

    def remote(src, dst, send, recv, device):
        return pltpu.make_async_remote_copy(
            src_ref=src, dst_ref=dst, send_sem=send, recv_sem=recv, device_id=device, device_id_type=MESH
        )

    def loop(lo, hi, body):
        def run(k, carry):
            body(k)
            return carry

        lax.fori_loop(lo, hi, run, 0)

    def done(ref, sem):
        pltpu.make_async_copy(ref, ref, sem).wait()

    def spread(value):
        return jnp.concatenate([value] * (WIDE // LANES), axis=-1)

    block = min(BLOCK, x_ref.shape[0])
    blocks = x_ref.shape[0] // block
    pairs = [(rows.at[0], rows_ref), (lower.at[0], v_ref)]
    for k in range(blocks):
        pairs.append((features.at[0, pl.ds(k * block, block)], x_ref.at[pl.ds(k * block, block)]))
    pairs += [(head.at[0], w_ref), (targets.at[0], t_ref)]
    copies = load_all(pairs, load_sems)
    barrier = pltpu.get_barrier_semaphore()
    loop(1, plane, lambda d: pl.semaphore_signal(barrier, inc=1, device_id=ahead(d), device_id_type=MESH))
    loop(1, nb, lambda e: pl.semaphore_signal(barrier, inc=1, device_id=along(e), device_id_type=MESH))
    copies[0].wait()
    count_draws(rows_ref, m_ref)
    copies[1].wait()
    for k in range(blocks):
        copies[2 + k].wait()
        if k == blocks - 1:
            for copy in copies[2 + blocks :]:
                copy.wait()
        here = pl.ds(k * block, block)
        hh_ref[here], hl_ref[here] = split(jnp.tanh(product(x_ref[here], v_ref[...], NN)))

    def meta_copy(d):
        return remote(mine, meta.at[d - 1], meta_send, meta_recv, ahead(d))

    def copy1(h, d):
        peer = ahead(d)
        at = pl.multiple_of((peer[0] * nx + peer[2]) * share, share)
        return remote(delta.at[h, pl.ds(at, share)], got1.at[h, d - 1], send1.at[h], recv1.at[h], peer)

    drawn = rows_ref.shape[1]
    rate = -LR / drawn
    h = 0
    places = []
    start = w_ref[...].T
    errors(0, start, slice(0, outs), m_ref, t_ref, hh_ref, hl_ref, e_ref)
    first = gradient(outs, slice(None), hh_ref, hl_ref, e_ref) * rate
    pl.semaphore_wait(barrier, plane - 1 + nb - 1)
    loop(1, plane, lambda d: meta_copy(d).start())
    for col in range(0, outs, WIDE):
        columns = slice(col, col + WIDE)
        errors(1, (start + first)[columns], columns, m_ref, t_ref, hh_ref, hl_ref, e_ref)
        for row in range(0, hid, half):
            change = gradient(WIDE, slice(row, row + half), hh_ref, hl_ref, e_ref) * rate
            delta[h] = (first[columns, row : row + half] + change).T
            places.append((row, col))
            for d in order:
                copy1(h, d).start()
            h += 1

    done(meta, meta_recv)
    part[...] = mine[...] + jnp.sum(meta[...], axis=0)

    def part_copy(e):
        return remote(part, parts.at[e - 1], part_send, part_recv, along(e))

    loop(1, nb, lambda e: part_copy(e).start())

    def copy2(h, e):
        peer = along(e)
        return remote(sums.at[h, peer[1]], got2.at[h, e - 1], send2.at[h], recv2.at[h], peer)

    def copy3(h, e):
        return remote(totals.at[h, b], totals.at[h, b], send3.at[h], recv3.at[h], along(e))

    def target(h):
        row, col = places[h]
        return out.at[pl.ds(row + own, share), pl.ds(col, WIDE)]

    def copy4(h, d):
        return remote(picked.at[h, d - 1], target(h), send4.at[h], recv4.at[h], behind(d))

    def stage1(h):
        done(got1.at[h], recv1.at[h])
        value = delta[h, pl.ds(own, share)]
        got = got1[h]
        for k in range(CLUSTERS):
            sums[h, k] = value * spread(mine[pl.ds(k, 1), :]) + jnp.sum(got * spread(meta[:, k : k + 1, :]), axis=0)
        for e in z_order:
            copy2(h, e).start()

    def stage2(h):
        done(got2.at[h], recv2.at[h])
        totals[h, b] = sums[h, b] + jnp.sum(got2[h], axis=0)
        for e in z_order:
            copy3(h, e).start()

    def stage3(h, scale):
        done(got2.at[h], recv3.at[h])
        value = jnp.zeros(picked.shape[1:], jnp.float32)
        kept = jnp.zeros((share, WIDE), jnp.float32)
        for k in range(CLUSTERS):
            mean = totals[h, k] * spread(scale[k : k + 1, :])
            value = jnp.where(spread(meta[:, k : k + 1, :]) > 0.0, mean[None], value)
            kept = jnp.where(spread(mine[pl.ds(k, 1), :]) > 0.0, mean, kept)
        picked[h] = value
        for d in order:
            copy4(h, d).start()
        row, col = places[h]
        out[pl.ds(row + own, share), pl.ds(col, WIDE)] = kept

    for h in range(chunks):
        stage1(h)
    for h in range(chunks):
        stage2(h)
    done(parts, part_recv)
    scale = 1.0 / (LR * (part[...] + jnp.sum(parts[...], axis=0)))
    for h in range(chunks):
        stage3(h, scale)
    done(meta, meta_send)
    done(parts, part_send)
    for h in range(chunks):
        done(got1.at[h], send1.at[h])
        done(got2.at[h], send2.at[h])
        done(got2.at[h], send3.at[h])
        done(got1.at[h], send4.at[h])

    for h in range(chunks):
        done(got1.at[h], recv4.at[h])


def on_device(sizes, features, targets, lower_weight, head_weight, batch_rows, sample_counts, cluster_ids):
    nc, nb, nx = sizes
    plane = nc * nx
    _, pool, inside = features.shape
    _, hid, outs = head_weight.shape
    _, steps, drawn = batch_rows.shape
    share = SUBLANES
    chunks = hid // (plane * share) * (outs // WIDE)
    blocks = pool // min(BLOCK, pool)
    hbm = pl.BlockSpec(memory_space=pltpu.HBM)
    vmem = pl.BlockSpec(memory_space=pltpu.VMEM)
    dma = pltpu.SemaphoreType.DMA
    f32, bf16 = jnp.float32, jnp.bfloat16
    place = lax.broadcasted_iota(jnp.int32, (CLUSTERS, LANES), 0) == cluster_ids[0]
    mine = jnp.where(place, sample_counts[0].astype(f32), 0.0)
    held = [
        pltpu.with_memory_space_constraint(v, pltpu.HBM)
        for v in (features, targets, lower_weight, head_weight, batch_rows)
    ]
    result = pl.pallas_call(
        functools.partial(kernel, sizes),
        out_shape=jax.ShapeDtypeStruct((hid, outs), f32),
        in_specs=[hbm] * 5 + [vmem],
        out_specs=vmem,
        scratch_shapes=[
            pltpu.VMEM((pool, inside), bf16),
            pltpu.VMEM((pool, outs), bf16),
            pltpu.VMEM((inside, hid), bf16),
            pltpu.VMEM((hid, outs), f32),
            pltpu.VMEM((pool, hid), bf16),
            pltpu.VMEM((pool, hid), bf16),
            pltpu.VMEM((2 * outs, pool), bf16),
            pltpu.VMEM((steps, pool // LANES, LANES), f32),
            pltpu.VMEM((steps, drawn), jnp.int32),
            pltpu.VMEM((chunks, plane * share, WIDE), f32),
            pltpu.VMEM((plane - 1, CLUSTERS, LANES), f32),
            pltpu.VMEM((CLUSTERS, LANES), f32),
            pltpu.VMEM((nb - 1, CLUSTERS, LANES), f32),
            pltpu.VMEM((chunks, plane - 1, share, WIDE), f32),
            pltpu.VMEM((chunks, CLUSTERS, share, WIDE), f32),
            pltpu.VMEM((chunks, nb - 1, share, WIDE), f32),
            pltpu.VMEM((chunks, CLUSTERS, share, WIDE), f32),
            pltpu.VMEM((chunks, plane - 1, share, WIDE), f32),
            dma((blocks + 4,)),
            dma, dma, dma, dma,
            *[dma((chunks,)) for _ in range(8)],
        ],
        compiler_params=pltpu.CompilerParams(
            collective_id=0, has_side_effects=True, vmem_limit_bytes=GRANT
        ),
    )(*held, mine)
    return result[None]


def solution(mesh):
    sizes = tuple(mesh.shape[a] for a in AXES)
    whole = P(AXES)
    matrix = P(AXES, None, None)
    return jax.shard_map(
        functools.partial(on_device, sizes),
        mesh=mesh,
        in_specs=(matrix, matrix, matrix, matrix, matrix, whole, whole),
        out_specs=matrix,
        check_vma=False,
    )
```
